32 devices in a mesh: tile: 8 (over z, y), mem: 4 (over x, core).
Axes of the slice: x: 2, y: 2, z: 4, core: 2. Of those that a mesh axis runs over, the one named last changes fastest.
Arguments:
- background: bfloat16 [112, 80, 512], P('tile', 'mem'), may hold values from -6 to 6
- obs_ens: bfloat16 [112, 80, 128], P('tile', 'mem'), may hold values from -6 to 6
- innovation: float32 [112, 128], P('tile'), may hold values from -6 to 6
- precision: float32 [112, 128], P('tile'), may hold values from 0.1 to 2
- loc_weight: float32 [112, 7], P('tile'), may hold values from 0.1 to 1
- old_split: int32 [9], replicated, may hold values from 0 to 64, as said below
- new_split: int32 [9], replicated, may hold values from 0 to 64, as said below
- obs_count: int32 [112], P('tile'), may hold values from 32 to 128
- halo_tiles: int32 [8, 12], replicated, may hold values from 0 to 63, as said below
- region_list: int32 [112, 7], P('tile'), may hold values from 0 to 25, as said below
Outputs:
- analysis: bfloat16 [112, 80, 512], P('tile', 'mem')
The draws below stay inside these ranges and needn't reach their ends.
Inputs may be any that keep to these rules, and one draw needn't show every extreme that they name: old_split[0] = 0 and old_split[8] = 64; each device holds between 2 and 14 old tiles, exactly 14 on some device. new_split[0] = 0 and new_split[8] = 64; each device holds between 6 and 10 new tiles; every new_split[d] differs from old_split[d] by at most 2, by exactly 2 for some d. `halo_tiles`: row d is 3 groups of 4 entries; a group holds distinct tiles in rising order that one device p other than d holds under new_split, with p within 3 of d, and the 3 devices of a row are distinct. `region_list`: for a slot of device d, an entry r < 14 names d's slot r, which is live; an entry r >= 14 names the tile halo_tiles[d, r - 14].
All inputs are finite; a program needn't handle non-finite values.
Results may differ from the reference program's by a relative error of at most 0.0057.
Values may be sent and summed in bfloat16 or wider, within the bound.
A program may use at most 64 MiB of HBM per device.

```python
import math
import jax
import jax.numpy as jnp
from jax import lax

MEMBERS = 80
STATE = 512
OBS_T = 128
TILE_MEAN = 8
CAP = 14
JITTER = 3
MOVE = 2
TILES = 64
SLOTS = 112
REACH = 3
HPEER = 3
HCAP = 4
HLIST = 12
NBR = 7
NS_ITERS = 6
N_TILE = 8


def split_pair(key):
    inner_key = jax.random.fold_in(key, 11)
    jitter_key, widest_key = jax.random.split(inner_key)
    boundary = jnp.arange(N_TILE + 1, dtype=jnp.int32)
    jitter = jax.random.randint(jitter_key, (N_TILE + 1,), -JITTER, JITTER + 1)
    widest = jax.random.randint(widest_key, (), 1, N_TILE - 1)
    jitter = jnp.where(boundary == widest, -JITTER, jitter)
    jitter = jnp.where(boundary == widest + 1, JITTER, jitter)
    jitter = jnp.where((boundary == 0) | (boundary == N_TILE), 0, jitter)
    old_bounds = boundary * TILE_MEAN + jitter
    moved_by = jnp.clip(jitter, -MOVE, MOVE)
    new_bounds = old_bounds - moved_by
    return (old_bounds.astype(jnp.int32), new_bounds.astype(jnp.int32))


def draw_old_split(key, part):
    return split_pair(key)[0]


def draw_new_split(key, part):
    return split_pair(key)[1]


def draw_halo_tiles(key, part):
    old_bounds, new_bounds = split_pair(key)
    inner_key = jax.random.fold_in(key, 23)
    peer_key, slot_key = jax.random.split(inner_key)
    offsets = jnp.concatenate([jnp.arange(-REACH, 0), jnp.arange(1, REACH + 1)]).astype(jnp.int32)
    device = jnp.arange(N_TILE, dtype=jnp.int32)
    target = device[:, None] + offsets[None, :]
    inside = (target >= 0) & (target < N_TILE)
    scores = jax.random.randint(peer_key, (N_TILE, 2 * REACH), 0, 1 << 20) * (2 * REACH) + jnp.arange(2 * REACH)[None, :]
    scores = jnp.where(inside, scores, (1 << 30) + jnp.arange(2 * REACH)[None, :])
    ranking = jnp.argsort(scores, axis=1, stable=True)[:, :HPEER]
    peer_ids = jnp.take_along_axis(target, ranking, axis=1)
    counts = new_bounds[1:] - new_bounds[:-1]
    peer_count = counts[peer_ids]
    slot_scores = jax.random.randint(slot_key, (N_TILE, HPEER, CAP), 0, 1 << 20) * CAP + jnp.arange(CAP)[None, None, :]
    slot_scores = jnp.where(jnp.arange(CAP)[None, None, :] < peer_count[:, :, None], slot_scores, (1 << 30) + jnp.arange(CAP)[None, None, :])
    chosen = jnp.sort(jnp.argsort(slot_scores, axis=2, stable=True)[:, :, :HCAP], axis=2)
    positions = new_bounds[peer_ids][:, :, None] + chosen
    return positions.reshape(N_TILE, HLIST).astype(jnp.int32)


def draw_region_list(key, part):
    old_bounds, new_bounds = split_pair(key)
    inner_key = jax.random.fold_in(key, 37)
    kind_key, own_key, far_key = jax.random.split(inner_key, 3)
    counts = new_bounds[1:] - new_bounds[:-1]
    count_per_slot = jnp.repeat(counts, CAP, total_repeat_length=N_TILE * CAP)
    own_pick = jax.random.randint(own_key, (N_TILE * CAP, NBR), 0, 1 << 20) % count_per_slot[:, None]
    far_pick = CAP + jax.random.randint(far_key, (N_TILE * CAP, NBR), 0, HLIST)
    choose_far = jax.random.randint(kind_key, (N_TILE * CAP, NBR), 0, 2)
    return jnp.where(choose_far == 1, far_pick, own_pick).astype(jnp.int32)


def place_ends(array, rng, low, high):
    longest = array.shape.index(max(array.shape))
    spots = []
    for shift in (0, 1):
        where = [jax.random.randint(jax.random.fold_in(rng, axis), (), 0, length) for axis, length in enumerate(array.shape)]
        where[longest] = (where[longest] + shift) % array.shape[longest]
        spots.append(tuple(where))
    return array.at[spots[0]].set(low).at[spots[1]].set(high)


def block_scale(rng, dims, pieces, least, high):
    loudness = 1.0
    for dim, parts in pieces:
        steps = jax.random.uniform(jax.random.fold_in(jax.random.fold_in(rng, 6), dim), (parts,), jnp.float32, least / len(pieces), high / len(pieces))
        loudness = loudness * jnp.repeat(jnp.exp(steps), dims[dim] // parts).reshape((-1,) + (1,) * (len(dims) - 1 - dim))
    return loudness


def noise(key, extent, scale, reach, cuts=(), held_as=jnp.bfloat16):
    level = block_scale(key, extent, cuts, -0.22, 0.18) if cuts else 1.0
    values = jax.random.normal(key, extent, jnp.float32) * scale * level
    return jnp.minimum(jnp.maximum(values, -reach), reach).astype(held_as)


def setup_inputs(seed: int = 0) -> dict:
    arg_keys = jax.random.split(jax.random.key(seed), 11)
    background = noise(arg_keys[0], (SLOTS, MEMBERS, STATE), 1.0, 6.0, ((0, 8), (1, 4)))
    obs_ens = noise(arg_keys[1], (SLOTS, MEMBERS, OBS_T), 1.0, 6.0, ((0, 8), (1, 4)))
    innovation = noise(arg_keys[2], (SLOTS, OBS_T), 1.0, 6.0, ((0, 8),), jnp.float32)
    precision = jnp.clip(jnp.exp(math.log(2.0) - 2.9957323 * jax.random.uniform(arg_keys[3], (SLOTS, OBS_T), jnp.float32) ** block_scale(arg_keys[3], (SLOTS, OBS_T), ((0, 8),), -0.2, 0.2)), 0.1, 2.0)
    loc_weight = jnp.clip(jnp.exp(math.log(1.0) - 2.3025851 * jax.random.uniform(arg_keys[4], (SLOTS, NBR), jnp.float32) ** block_scale(arg_keys[4], (SLOTS, NBR), ((0, 8),), -0.2, 0.2)), 0.1, 1.0)
    old_split = draw_old_split(jax.random.fold_in(arg_keys[10], 71), 0)
    new_split = draw_new_split(jax.random.fold_in(arg_keys[10], 71), 0)
    obs_count = place_ends(jax.random.randint(arg_keys[7], (SLOTS,), OBS_T // 4, OBS_T + 1), jax.random.fold_in(arg_keys[7], 1), OBS_T // 4, OBS_T).astype(jnp.int32)
    halo_tiles = draw_halo_tiles(jax.random.fold_in(arg_keys[10], 71), 0)
    region_list = draw_region_list(jax.random.fold_in(arg_keys[10], 71), 0)
    return dict(background=background, obs_ens=obs_ens, innovation=innovation, precision=precision, loc_weight=loc_weight, old_split=old_split, new_split=new_split, obs_count=obs_count, halo_tiles=halo_tiles, region_list=region_list)


inflation = 1.1
exact = lax.Precision.HIGHEST

def owner_of(split_points, position):
    bounds = split_points[1:]
    return lax.optimization_barrier(jnp.sum((bounds[None, :] <= position[:, None]).astype(jnp.int32), axis=1)).astype(jnp.int32)

def inverse_root(system, repeats):
    identity = jnp.eye(system.shape[-1], dtype=system.dtype)
    frobenius = jnp.sqrt(lax.optimization_barrier(jnp.sum(system * system, axis=(1, 2))))
    root_part = system / frobenius[:, None, None]
    inverse_part = jnp.broadcast_to(identity, system.shape)
    for repeat in range(repeats):
        middle = 0.5 * (3.0 * identity - jnp.einsum('pij,pjk->pik', inverse_part, root_part, precision=exact))
        root_part = jnp.einsum('pij,pjk->pik', root_part, middle, precision=exact)
        inverse_part = jnp.einsum('pij,pjk->pik', middle, inverse_part, precision=exact)
    return (inverse_part, frobenius)

def reference(background, obs_ens, innovation, precision, loc_weight, old_split, new_split, obs_count, halo_tiles, region_list):
    slot_all = jnp.arange(N_TILE * CAP, dtype=jnp.int32)
    device = (slot_all // CAP).astype(jnp.int32)
    within = (slot_all % CAP).astype(jnp.int32)
    tile_pos = new_split[device] + within
    live_slot = tile_pos < new_split[device + 1]
    safe_pos = jnp.minimum(tile_pos, TILES - 1).astype(jnp.int32)
    old_owner = owner_of(old_split, safe_pos)
    old_slot = (old_owner * CAP + safe_pos - old_split[old_owner]).astype(jnp.int32)
    live_obs = (jnp.arange(OBS_T, dtype=jnp.int32)[None, :] < obs_count[:, None]).astype(jnp.float32)
    root_weight = jnp.sqrt(precision * live_obs)
    scaled = (obs_ens.astype(jnp.float32) * root_weight[:, None, :]).astype(jnp.bfloat16)
    pulled = (root_weight * innovation).astype(jnp.bfloat16)
    flat_halo = halo_tiles.reshape(-1)
    halo_owner = owner_of(new_split, flat_halo)
    halo_slot = (halo_owner * CAP + flat_halo - new_split[halo_owner]).astype(jnp.int32).reshape(N_TILE, HLIST)
    own_slot = device[:, None] * CAP + region_list
    far_slot = halo_slot[device[:, None], jnp.clip(region_list - CAP, 0, HLIST - 1)]
    entry_slot = jnp.where(region_list < CAP, own_slot, far_slot).astype(jnp.int32)
    entry_slot = jnp.concatenate([slot_all[:, None], entry_slot], axis=1)
    entry_weight = jnp.concatenate([jnp.ones((N_TILE * CAP, 1), jnp.float32), loc_weight], axis=1)

    def one_device(device_index):
        slot_ids = (device_index * CAP + jnp.arange(CAP, dtype=jnp.int32)).astype(jnp.int32)
        region_rows = entry_slot[slot_ids]
        row_weights = entry_weight[slot_ids]
        region = scaled[region_rows].astype(jnp.float32)
        region_pulled = pulled[region_rows].astype(jnp.float32)
        products = jnp.einsum('pekn,pejn->pekj', region, region, precision=exact)
        gram_matrix = lax.optimization_barrier(jnp.sum(row_weights[:, :, None, None] * products, axis=1))
        pull_terms = jnp.einsum('pekn,pen->pek', region, region_pulled, precision=exact)
        pull_sum = lax.optimization_barrier(jnp.sum(row_weights[:, :, None] * pull_terms, axis=1))
        identity = jnp.eye(MEMBERS, dtype=jnp.float32)
        system = gram_matrix + (MEMBERS - 1) / inflation * identity
        inverse, frobenius = inverse_root(system, NS_ITERS)
        spread = (math.sqrt(MEMBERS - 1) / jnp.sqrt(frobenius))[:, None, None] * inverse
        half_way = jnp.einsum('pij,pj->pi', inverse, pull_sum, precision=exact)
        mean_weight = jnp.einsum('pij,pj->pi', inverse, half_way, precision=exact) / frobenius[:, None]
        transform = (spread + mean_weight[:, :, None]).astype(jnp.bfloat16).astype(jnp.float32)
        state_rows = background[old_slot[slot_ids]].astype(jnp.float32)
        mean_state = lax.optimization_barrier(jnp.sum(state_rows, axis=1)) / MEMBERS
        keep_share = 1.0 - lax.optimization_barrier(jnp.sum(transform, axis=1))
        analysis_rows = jnp.einsum('pij,pis->pjs', transform, state_rows, precision=exact) + keep_share[:, :, None] * mean_state[:, None, :]
        return jnp.where(live_slot[slot_ids][:, None, None], analysis_rows, 0.0).astype(jnp.bfloat16)
    result = lax.map(one_device, jnp.arange(N_TILE, dtype=jnp.int32))
    return result.reshape(N_TILE * CAP, MEMBERS, STATE)
```

```python
import functools
import math

import jax
import jax.numpy as jnp
from jax import lax
from jax.experimental import pallas as pl
from jax.experimental.pallas import tpu as pltpu
from jax.sharding import PartitionSpec as P

TILE_MEAN = 8
CORES = 2
MOVE = 2
REACH = 3
HPEER = 3
HCAP = 4
NS_ITERS = 6
LIVE_MAX = TILE_MEAN + MOVE
INFLATION = 1.1
PAD = 24
MESH = pl.DeviceIdType.MESH
F32 = jnp.float32
BF16 = jnp.bfloat16
LANES = 128
OFFSETS = tuple(range(-REACH, 0)) + tuple(range(1, REACH + 1))


def dot(a, b):
    return jnp.dot(a, b, preferred_element_type=F32)


def cut(a):
    high = a.astype(BF16)
    return high, (a - high.astype(F32)).astype(BF16)


def kernel(
    devices,
    ranks,
    old_hbm,
    new_hbm,
    count_hbm,
    halo_hbm,
    region_hbm,
    weight_hbm,
    back_hbm,
    obs_hbm,
    innov_hbm,
    prec_hbm,
    out_ref,
    old_ref,
    new_ref,
    count_ref,
    halo_ref,
    region_ref,
    weight_ref,
    back_ref,
    obs_ref,
    innov_ref,
    prec_ref,
    mine,
    back_t,
    table,
    stage,
    arrived,
    mig_out,
    mig_in,
    states,
    gram_s,
    yz_s,
    t_full,
    t_all,
    load_sem,
    halo_send,
    halo_recv,
    mig_send,
    mig_recv,
    own_send,
    own_recv,
    far_send,
    far_recv,
    early_send,
    early_recv,
    state_send,
    state_recv,
    t_send,
    t_recv,
):
    members, capacity, width = back_ref.shape
    obs_slots = obs_ref.shape[2]
    ensemble = members * ranks
    full = PAD * ranks
    halo_count = HPEER * HCAP
    per_core = -(-LIVE_MAX // CORES)
    me = lax.axis_index("tile")
    rank = lax.axis_index("mem")
    core = lax.rem(rank, CORES)
    chip = rank // CORES
    pair = rank + 1 - 2 * core
    half_ranks = ranks // CORES
    peers = [lax.rem(rank + j, ranks) for j in range(1, ranks)]

    barrier = pltpu.get_barrier_semaphore()
    for offset in OFFSETS:
        target = me + offset

        @pl.when((target >= 0) & (target < devices))
        def _():
            pl.semaphore_signal(barrier, inc=1, device_id=(target, rank), device_id_type=MESH)

    for peer in peers:
        pl.semaphore_signal(barrier, inc=1, device_id=(me, peer), device_id_type=MESH)

    loads = {}
    for k, (name, src, dst) in enumerate((
        ("count", count_hbm, count_ref),
        ("obs", obs_hbm, obs_ref),
        ("prec", prec_hbm, prec_ref),
        ("innov", innov_hbm, innov_ref),
        ("new", new_hbm, new_ref),
        ("halo", halo_hbm, halo_ref),
        ("back", back_hbm, back_ref),
        ("old", old_hbm, old_ref),
        ("region", region_hbm, region_ref),
        ("weight", weight_hbm, weight_ref),
    )):
        loads[name] = pltpu.make_async_copy(src, dst, load_sem.at[k])
        loads[name].start()

    row_id = lax.broadcasted_iota(jnp.int32, (PAD, obs_slots), 0)
    lane_id = lax.broadcasted_iota(jnp.int32, (1, obs_slots), 1)

    for s in range(LIVE_MAX):
        states[s, rank] = jnp.zeros((PAD, width), BF16)
    for b in range(per_core):
        yz_s[b, 2 * full :] = jnp.zeros((LANES - full, 2 * LANES), BF16)

    for name in ("count", "obs", "prec", "innov"):
        loads[name].wait()
    obs_all = obs_ref[...].astype(F32)
    for s in range(LIVE_MAX):
        live = (lane_id < count_ref[s]).astype(F32)
        root = jnp.sqrt(prec_ref[s : s + 1, :] * live)
        pulled = root * innov_ref[s : s + 1, :]
        rows = obs_all[:, s, :] * root
        fill = jnp.zeros((PAD - members, obs_slots), F32)
        block = jnp.concatenate([rows, fill], axis=0)
        block = jnp.where(row_id == members, pulled, block).astype(BF16)
        mine[s] = block
        table[s, rank] = block

    loads["new"].wait()
    loads["halo"].wait()
    new_start, new_end = new_ref[me], new_ref[me + 1]
    for k, offset in enumerate(OFFSETS):
        reader = jnp.clip(me + offset, 0, devices - 1)
        for c in range(HCAP):
            index = jnp.int32(0)
            for g in range(HPEER):
                first = halo_ref[reader, g * HCAP]
                here = (first >= new_start) & (first < new_end)
                index += jnp.where(here, halo_ref[reader, g * HCAP + c] - new_start, 0)
            index = jnp.clip(index, 0, LIVE_MAX - 1)
            stage[k, c] = mine[index]

    signals = ranks - 1
    for offset in OFFSETS:
        inside = (me + offset >= 0) & (me + offset < devices)
        signals += jnp.where(inside, 1, 0)
    pl.semaphore_wait(barrier, signals)

    def remote(src, dst, send, recv, target):
        return pltpu.make_async_remote_copy(
            src_ref=src,
            dst_ref=dst,
            send_sem=send,
            recv_sem=recv,
            device_id=target,
            device_id_type=MESH,
        )

    halo_copies = []
    for k, offset in enumerate(OFFSETS):
        back_slot = len(OFFSETS) - 1 - k
        halo_copies.append(remote(
            stage.at[k], arrived.at[back_slot], halo_send.at[k], halo_recv.at[back_slot],
            (me + offset, rank),
        ))
    for k in sorted(range(len(OFFSETS)), key=lambda i: -abs(OFFSETS[i])):
        target = me + OFFSETS[k]

        @pl.when((target >= 0) & (target < devices))
        def _(copy=halo_copies[k]):
            copy.start()

    def gather(piece, send, recv):
        here = piece(rank)
        direct = [remote(here, here, send.at[0], recv.at[0], (me, pair))]
        passed = []
        for j in range(1, half_ranks):
            ahead = lax.rem(rank + CORES * j, ranks)
            behind = piece(lax.rem(rank + ranks - CORES * j, ranks))
            direct.append(remote(here, here, send.at[j], recv.at[j], (me, ahead)))
            k = half_ranks + j - 1
            passed.append(remote(behind, behind, send.at[k], recv.at[k], (me, pair)))
        return direct, passed

    def start(copies):
        for copy in copies:
            copy.start()

    def arrive(copies):
        for copy in copies:
            copy.wait_recv()

    own_rows = pl.ds(0, LIVE_MAX)
    own_copies, own_passed = gather(lambda r: table.at[own_rows, r], own_send, own_recv)
    start(own_copies[::-1])

    loads["back"].wait()
    loads["old"].wait()
    old_start, old_end = old_ref[me], old_ref[me + 1]
    back_all = back_ref[...].astype(F32)
    for s in range(capacity):
        back_t[s] = back_all[:, s, :].astype(BF16)
    old_count = old_end - old_start
    for c in range(MOVE):
        mig_out[0, c] = back_t[jnp.clip(c, 0, capacity - 1)]
        mig_out[1, c] = back_t[jnp.clip(old_count - MOVE + c, 0, capacity - 1)]
    mig_copies = []
    for side, offset in ((0, -1), (1, 1)):
        target = me + offset
        copy = remote(
            mig_out.at[side], mig_in.at[1 - side], mig_send.at[side], mig_recv.at[1 - side],
            (target, rank),
        )
        mig_copies.append(copy)

        @pl.when((target >= 0) & (target < devices))
        def _(copy=copy):
            copy.start()

    early = range(MOVE, TILE_MEAN - 2 * MOVE)
    for s in early:
        states[s, rank, :members] = back_t[jnp.clip(new_start + s - old_start, 0, capacity - 1)]
    early_rows = pl.ds(early.start, len(early))
    early_copies, early_passed = gather(lambda r: states.at[early_rows, r], early_send, early_recv)
    start(early_copies[::-1])

    arrive(own_copies[1:])
    start(own_passed)

    for k, offset in enumerate(OFFSETS):
        back_slot = len(OFFSETS) - 1 - k
        source = me + OFFSETS[back_slot]

        @pl.when((source >= 0) & (source < devices))
        def _(copy=halo_copies[k]):
            copy.wait_recv()

    far = []
    for g in range(HPEER):
        first = halo_ref[me, g * HCAP]
        owner = jnp.int32(0)
        for k, offset in enumerate(OFFSETS):
            source = jnp.clip(me + offset, 0, devices - 1)
            held = (first >= new_ref[source]) & (first < new_ref[source + 1])
            inside = (me + offset >= 0) & (me + offset < devices)
            owner = jnp.where(held & inside, k, owner)
        for c in range(HCAP):
            table[LIVE_MAX + g * HCAP + c, rank] = arrived[owner, c]
        rows = pl.ds(LIVE_MAX + g * HCAP, HCAP)
        far.append(gather(lambda r, rows=rows: table.at[rows, r], far_send.at[g], far_recv.at[g]))
        start(far[g][0][::-1])

    for side, offset in ((0, -1), (1, 1)):
        source = me - offset

        @pl.when((source >= 0) & (source < devices))
        def _(copy=mig_copies[side]):
            copy.wait_recv()

    late = []
    for first, last in ((early.stop, LIVE_MAX), (0, early.start)):
        for s in range(first, last):
            position = new_start + s
            left = mig_in[0, jnp.clip(position - old_start + MOVE, 0, MOVE - 1)]
            own = back_t[jnp.clip(position - old_start, 0, capacity - 1)]
            right = mig_in[1, jnp.clip(position - old_end, 0, MOVE - 1)]
            row = jnp.where(position < old_start, left, jnp.where(position < old_end, own, right))
            states[s, rank, :members] = row
        rows = pl.ds(first, last - first)
        k = len(late)
        late.append(gather(lambda r, rows=rows: states.at[rows, r], state_send.at[k], state_recv.at[k]))
        start(late[k][0][::-1])

    arrive(early_copies[1:])
    start(early_passed)
    arrive(own_copies[:1] + own_passed)

    blank = jnp.zeros((LANES - full, obs_slots), BF16)

    def product(index):
        block = table[index].reshape(full, obs_slots)
        wide = jnp.concatenate([block, blank], axis=0)
        gram_s[index] = lax.dot_general(
            block, wide, (((1,), (1,)), ((), ())), preferred_element_type=F32
        )

    for s in range(LIVE_MAX):
        product(s)

    for g in range(HPEER):
        arrive(far[g][0][1:])
        start(far[g][1])
    for g in range(HPEER):
        arrive(far[g][0][:1] + far[g][1])
        for c in range(HCAP):
            product(LIVE_MAX + g * HCAP + c)

    shape = (full, LANES)
    grid_row = lax.broadcasted_iota(jnp.int32, shape, 0)
    grid_col = lax.broadcasted_iota(jnp.int32, shape, 1)
    live_row = lax.rem(grid_row, PAD) < members
    live_col = (lax.rem(grid_col, PAD) < members) & (grid_col < full)
    rider = grid_row == members
    live = live_row & live_col
    kept = (live_row | rider) & live_col
    unit = jnp.where(live & (grid_row == grid_col), 1.0, 0.0)
    half_unit = 1.5 * unit
    shift = (ensemble - 1) / INFLATION
    loads["region"].wait()
    loads["weight"].wait()
    entries = region_ref.shape[0]
    fill = jnp.zeros((LANES - full, LANES), BF16)

    def tall(a):
        return jnp.concatenate([a, fill], axis=0)

    def times(left, high, low):
        both = jnp.concatenate([high, high], axis=0)
        return dot(left, both) + dot(left[:, :LANES], low)

    def wide(a):
        high, low = cut(a)
        return jnp.concatenate([high, low], axis=1)

    norms = []
    for b in range(per_core):
        slot = jnp.minimum(CORES * b + core, LIVE_MAX - 1)
        gram = gram_s[slot]
        for e in range(entries):
            named = region_ref[e, slot]
            index = jnp.where(named < capacity, named, named - capacity + LIVE_MAX)
            index = jnp.clip(index, 0, LIVE_MAX + halo_count - 1)
            gram += weight_ref[e, slot] * gram_s[index]
        system = jnp.where(kept, gram, 0.0) + shift * unit
        square = jnp.where(live, system * system, 0.0)
        total = jnp.sum(jnp.sum(square, axis=1, keepdims=True), axis=0, keepdims=True)
        norm = jnp.sqrt(total)
        norms.append(norm)
        y = system / norm
        middle = half_unit - 0.5 * jnp.where(live, y, 0.0)
        high, low = cut(middle)
        first = times(wide(y), tall(high), tall(low))
        yz_s[b, :full] = wide(jnp.where(rider, 0.0, first))
        yz_s[b, full : 2 * full] = wide(jnp.where(rider, first, middle))

    def cross(b):
        z = yz_s[b, full : 2 * full]
        return times(z, yz_s[b, :LANES, :LANES], yz_s[b, :LANES, LANES:])

    def step(_, carry):
        middles = []
        for b in range(per_core):
            high, low = cut(half_unit - 0.5 * cross(b))
            middles.append((tall(high), tall(low)))
        for b in range(per_core):
            yz_s[b, : 2 * full] = wide(times(yz_s[b, : 2 * full], *middles[b]))
        return carry

    lax.fori_loop(0, NS_ITERS - 2, step, 0)

    piece = CORES * PAD
    block = 16
    start_row = members // block * block
    middles, riders = [], []
    for b in range(per_core):
        high, low = cut(half_unit - 0.5 * cross(b))
        middles.append((tall(high), tall(low)))
        q = yz_s[b, full + start_row : full + start_row + block]
        z_rows = slice(full, full + LANES)
        riders.append(times(q, yz_s[b, z_rows, :LANES], yz_s[b, z_rows, LANES:]))
    for b in range(per_core):
        chosen = yz_s[b, pl.ds(pl.multiple_of(full + chip * piece, block), piece)]
        stack = jnp.concatenate([chosen, wide(riders[b])], axis=0)
        both = times(stack, *middles[b])
        lead = times(wide(both[piece:]), *middles[b])[members - start_row : members - start_row + 1]
        spread = math.sqrt(ensemble - 1) * lax.rsqrt(norms[b])
        t_full[:, b] = (spread * both[:piece] + lead).astype(BF16).reshape(CORES, PAD, LANES)

    other = 1 - core
    t_copy = remote(t_full.at[other], t_all.at[core], t_send, t_recv, (me, pair))
    t_copy.start()
    t_all[core] = t_full[core]

    for direct, passed in late:
        arrive(direct[1:])
        start(passed)
    arrive(early_copies[:1] + early_passed)
    for direct, passed in late:
        arrive(direct[:1] + passed)
    t_copy.wait_recv()

    piece_row = lax.broadcasted_iota(jnp.int32, (PAD, full), 0)
    for s in range(LIVE_MAX):
        weights = t_all[s % CORES, s // CORES][:, :full]
        weights = jnp.where(piece_row == members, jnp.ones_like(weights), weights)
        keep = 1.0 - jnp.sum(weights.astype(F32), axis=1, keepdims=True)
        blended = dot(weights, states[s].reshape(full, width))
        mean = blended[members : members + 1, :] / ensemble
        value = (blended + keep * mean)[:members]
        is_live = new_start + s < new_end
        out_ref[s] = jnp.where(is_live, value, 0.0).astype(BF16)
    for s in range(LIVE_MAX, capacity):
        out_ref[s] = jnp.zeros((members, width), BF16)

    for k, offset in enumerate(OFFSETS):
        target = me + offset

        @pl.when((target >= 0) & (target < devices))
        def _(copy=halo_copies[k]):
            copy.wait_send()

    for side, offset in ((0, -1), (1, 1)):
        target = me + offset

        @pl.when((target >= 0) & (target < devices))
        def _(copy=mig_copies[side]):
            copy.wait_send()

    gathers = own_copies + own_passed + early_copies + early_passed + [t_copy]
    for direct, passed in far + late:
        gathers += direct + passed
    for copy in gathers:
        copy.wait_send()


def shards(devices, ranks, background, obs_ens, innovation, precision, loc_weight, old_split,
           new_split, obs_count, halo_tiles, region_list):
    capacity, members, width = background.shape
    obs_slots = obs_ens.shape[2]
    full = PAD * ranks
    halo_count = HPEER * HCAP
    per_core = -(-LIVE_MAX // CORES)
    hbm = pl.BlockSpec(memory_space=pltpu.MemorySpace.HBM)
    vmem = pl.BlockSpec(memory_space=pltpu.VMEM)
    count = len(OFFSETS)
    dma = pltpu.SemaphoreType.DMA
    operands = (old_split, new_split, obs_count, halo_tiles, region_list.T, loc_weight.T,
                jnp.swapaxes(background, 0, 1), jnp.swapaxes(obs_ens, 0, 1), innovation, precision)
    spaces = [pltpu.SMEM] * 6 + [pltpu.VMEM] * 4
    return pl.pallas_call(
        functools.partial(kernel, devices, ranks),
        out_shape=pltpu.VMEM((capacity, members, width), BF16),
        in_specs=[hbm] * len(operands),
        out_specs=vmem,
        scratch_shapes=[space(x.shape, x.dtype) for space, x in zip(spaces, operands)] + [
            pltpu.VMEM((LIVE_MAX, PAD, obs_slots), BF16),
            pltpu.VMEM((capacity, members, width), BF16),
            pltpu.VMEM((LIVE_MAX + halo_count, ranks, PAD, obs_slots), BF16),
            pltpu.VMEM((count, HCAP, PAD, obs_slots), BF16),
            pltpu.VMEM((count, HCAP, PAD, obs_slots), BF16),
            pltpu.VMEM((2, MOVE, members, width), BF16),
            pltpu.VMEM((2, MOVE, members, width), BF16),
            pltpu.VMEM((LIVE_MAX, ranks, PAD, width), BF16),
            pltpu.VMEM((LIVE_MAX + halo_count, full, LANES), F32),
            pltpu.VMEM((per_core, full + LANES, 2 * LANES), BF16),
            pltpu.VMEM((CORES, per_core, PAD, LANES), BF16),
            pltpu.VMEM((CORES, per_core, PAD, LANES), BF16),
            dma((len(operands),)),
            dma((count,)),
            dma((count,)),
            dma((2,)),
            dma((2,)),
            dma((ranks - 1,)),
            dma((ranks - 1,)),
            dma((HPEER, ranks - 1)),
            dma((HPEER, ranks - 1)),
            dma((ranks - 1,)),
            dma((ranks - 1,)),
            dma((2, ranks - 1)),
            dma((2, ranks - 1)),
            dma,
            dma,
        ],
        compiler_params=pltpu.CompilerParams(
            collective_id=0, has_side_effects=True
        ),
        cost_estimate=pl.CostEstimate(flops=10**8, bytes_accessed=10**7, transcendentals=0),
    )(*operands)


def solution(mesh):
    in_specs = (
        P("tile", "mem", None),
        P("tile", "mem", None),
        P("tile", None),
        P("tile", None),
        P("tile", None),
        P(),
        P(),
        P("tile"),
        P(),
        P("tile", None),
    )
    out_specs = P("tile", "mem", None)
    body = functools.partial(shards, mesh.shape["tile"], mesh.shape["mem"])
    return jax.shard_map(body, mesh=mesh, in_specs=in_specs, out_specs=out_specs, check_vma=False)
```

```python
import functools
import math

import jax
import jax.numpy as jnp
from jax import lax
from jax.experimental import pallas as pl
from jax.experimental.pallas import tpu as pltpu
from jax.sharding import PartitionSpec as P

TILE_MEAN = 8
CORES = 2
MOVE = 2
REACH = 3
HPEER = 3
HCAP = 4
NS_ITERS = 6
LIVE_MAX = TILE_MEAN + MOVE
INFLATION = 1.1
PAD = 24
MESH = pl.DeviceIdType.MESH
F32 = jnp.float32
BF16 = jnp.bfloat16
LANES = 128
OFFSETS = tuple(range(-REACH, 0)) + tuple(range(1, REACH + 1))


def dot(a, b):
    return jnp.dot(a, b, preferred_element_type=F32)


def cut(a):
    high = a.astype(BF16)
    return high, (a - high.astype(F32)).astype(BF16)


def kernel(
    devices,
    ranks,
    old_hbm,
    new_hbm,
    count_hbm,
    halo_hbm,
    region_hbm,
    weight_hbm,
    back_hbm,
    obs_hbm,
    innov_hbm,
    prec_hbm,
    out_ref,
    old_ref,
    new_ref,
    count_ref,
    halo_ref,
    region_ref,
    weight_ref,
    back_ref,
    obs_ref,
    innov_ref,
    prec_ref,
    mine,
    back_t,
    table,
    stage,
    arrived,
    mig_out,
    mig_in,
    states,
    gram_s,
    yz_s,
    t_full,
    t_all,
    load_sem,
    halo_recv,
    mig_recv,
    own_recv,
    far_send,
    far_recv,
    state_send,
    state_recv,
    t_send,
    t_recv,
):
    members, capacity, width = back_ref.shape
    obs_slots = obs_ref.shape[2]
    ensemble = members * ranks
    full = PAD * ranks
    halo_count = HPEER * HCAP
    per_core = -(-LIVE_MAX // CORES)
    me = lax.axis_index("tile")
    rank = lax.axis_index("mem")
    core = lax.rem(rank, CORES)
    chip = rank // CORES
    pair = rank + 1 - 2 * core
    half_ranks = ranks // CORES

    def signal(sem, tile, to):
        pl.semaphore_signal(sem, inc=1, device_id=(tile, to), device_id_type=MESH)

    barrier = pltpu.get_barrier_semaphore()
    for offset in OFFSETS:

        @pl.when((me + offset >= 0) & (me + offset < devices))
        def _(offset=offset):
            signal(barrier, me + offset, rank)

    for j in range(1, ranks):
        signal(barrier, me, lax.rem(rank + j, ranks))

    loads = {}
    for k, (name, src, dst) in enumerate((
        ("count", count_hbm, count_ref),
        ("obs", obs_hbm, obs_ref),
        ("prec", prec_hbm, prec_ref),
        ("innov", innov_hbm, innov_ref),
        ("new", new_hbm, new_ref),
        ("halo", halo_hbm, halo_ref),
        ("back", back_hbm, back_ref),
        ("old", old_hbm, old_ref),
        ("region", region_hbm, region_ref),
        ("weight", weight_hbm, weight_ref),
    )):
        loads[name] = pltpu.make_async_copy(src, dst, load_sem.at[k])
        loads[name].start()

    row_id = lax.broadcasted_iota(jnp.int32, (PAD, obs_slots), 0)
    lane_id = lax.broadcasted_iota(jnp.int32, (1, obs_slots), 1)

    for s in range(LIVE_MAX):
        states[s, rank] = jnp.zeros((PAD, width), BF16)
    for b in range(per_core):
        yz_s[b, 2 * full :] = jnp.zeros((LANES - full, 2 * LANES), BF16)

    for name in ("count", "obs", "prec", "innov"):
        loads[name].wait()
    obs_all = obs_ref[...].astype(F32)
    for s in range(LIVE_MAX):
        live = (lane_id < count_ref[s]).astype(F32)
        root = jnp.sqrt(prec_ref[s : s + 1, :] * live)
        pulled = root * innov_ref[s : s + 1, :]
        rows = obs_all[:, s, :] * root
        fill = jnp.zeros((PAD - members, obs_slots), F32)
        block = jnp.concatenate([rows, fill], axis=0)
        block = jnp.where(row_id == members, pulled, block).astype(BF16)
        mine[s] = block
        table[s, rank] = block

    loads["new"].wait()
    loads["halo"].wait()
    loads["region"].wait()
    new_start, new_end = new_ref[me], new_ref[me + 1]
    def remote(src, dst, send, recv, target):
        return pltpu.make_async_remote_copy(
            src_ref=src,
            dst_ref=dst,
            send_sem=send,
            recv_sem=recv,
            device_id=target,
            device_id_type=MESH,
        )

    def fill_stage(k):
        reader = jnp.clip(me + OFFSETS[k], 0, devices - 1)
        for c in range(HCAP):
            index = jnp.int32(0)
            for g in range(HPEER):
                first = halo_ref[reader, g * HCAP]
                here = (first >= new_start) & (first < new_end)
                index += jnp.where(here, halo_ref[reader, g * HCAP + c] - new_start, 0)
            index = jnp.clip(index, 0, LIVE_MAX - 1)
            stage[k, c] = mine[index]

    halo_copies = []
    for k, offset in enumerate(OFFSETS):
        back_slot = len(OFFSETS) - 1 - k
        halo_copies.append(remote(
            stage.at[k], arrived.at[back_slot], load_sem.at[k], halo_recv.at[back_slot],
            (me + offset, rank),
        ))
    for k in range(len(OFFSETS)):
        fill_stage(k)
    pl.semaphore_wait(barrier, jnp.minimum(me, REACH) + jnp.minimum(devices - 1 - me, REACH) + ranks - 1)
    for k in sorted(range(len(OFFSETS)), key=lambda i: -abs(OFFSETS[i])):

        @pl.when((me + OFFSETS[k] >= 0) & (me + OFFSETS[k] < devices))
        def _(copy=halo_copies[k]):
            copy.start()

    def send_own(piece, send, ahead_recv, pair_recv):
        here = piece(rank)
        for j in range(1, half_ranks):
            ahead = lax.rem(rank + CORES * j, ranks)
            remote(here, here, send, ahead_recv, (me, ahead)).start()
        remote(here, here, send, pair_recv, (me, pair)).start()

    def send_passed(piece, send, pair_recv):
        for j in range(1, half_ranks):
            behind = piece(lax.rem(rank + ranks - CORES * j, ranks))
            remote(behind, behind, send, pair_recv, (me, pair)).start()

    def whole_of(piece, sem, count):
        block = piece(pl.ds(0, count))
        return pltpu.make_async_copy(block, block, sem)

    def arrive_ahead(piece, sem):
        whole_of(piece, sem, half_ranks - 1).wait()

    def arrive_pair(piece, sem):
        whole_of(piece, sem, half_ranks).wait()

    def own_piece(r):
        return table.at[0:LIVE_MAX, r]

    send_own(own_piece, load_sem.at[8], own_recv.at[0], own_recv.at[1])

    loads["back"].wait()
    loads["old"].wait()
    loads["weight"].wait()
    old_start, old_end = old_ref[me], old_ref[me + 1]
    back_all = back_ref[...].astype(F32)
    for s in range(capacity):
        back_t[s] = back_all[:, s, :].astype(BF16)
    old_count = old_end - old_start
    for c in range(MOVE):
        mig_out[0, c] = back_t[jnp.clip(c, 0, capacity - 1)]
        mig_out[1, c] = back_t[jnp.clip(old_count - MOVE + c, 0, capacity - 1)]
    mig_copies = []
    for side, offset in ((0, -1), (1, 1)):
        target = me + offset
        copy = remote(
            mig_out.at[side], mig_in.at[1 - side], load_sem.at[len(OFFSETS) + side], mig_recv.at[1 - side],
            (target, rank),
        )
        mig_copies.append(copy)

    @pl.when(me > 0)
    def _():
        mig_copies[0].start()

    early = range(MOVE, TILE_MEAN - 2 * MOVE)
    for s in early:
        states[s, rank, :members] = back_t[jnp.clip(new_start + s - old_start, 0, capacity - 1)]

    def early_piece(r):
        return states.at[early.start : early.stop, r]

    def first_piece(r):
        return states.at[0 : early.start, r]

    def last_piece(r):
        return states.at[early.stop : LIVE_MAX, r]

    def every_piece(r):
        return states.at[0:LIVE_MAX, r]

    send_own(early_piece, state_send, state_recv.at[0], state_recv.at[1])

    @pl.when(me + 1 < devices)
    def _():
        mig_copies[1].start()

    for k, offset in enumerate(OFFSETS):
        back_slot = len(OFFSETS) - 1 - k
        source = me + OFFSETS[back_slot]

        @pl.when((source >= 0) & (source < devices))
        def _(copy=halo_copies[k]):
            copy.wait_recv()

    far = []
    for g in range(HPEER):
        first = halo_ref[me, g * HCAP]
        owner = jnp.int32(0)
        for k, offset in enumerate(OFFSETS):
            source = jnp.clip(me + offset, 0, devices - 1)
            held = (first >= new_ref[source]) & (first < new_ref[source + 1])
            inside = (me + offset >= 0) & (me + offset < devices)
            owner = jnp.where(held & inside, k, owner)
        for c in range(HCAP):
            table[LIVE_MAX + g * HCAP + c, rank] = arrived[owner, c]
        first_row = LIVE_MAX + g * HCAP

        def far_piece(r, first_row=first_row):
            return table.at[first_row : first_row + HCAP, r]

        far.append(far_piece)
        send_own(far_piece, far_send.at[g], far_recv.at[0, g], far_recv.at[1, g])

    arrive_ahead(own_piece, own_recv.at[0])
    send_passed(own_piece, load_sem.at[8], own_recv.at[1])
    arrive_pair(own_piece, own_recv.at[1])

    blank = jnp.zeros((LANES - full, obs_slots), BF16)

    def product(index):
        block = table[index].reshape(full, obs_slots)
        wide = jnp.concatenate([block, blank], axis=0)
        gram_s[index] = lax.dot_general(
            block, wide, (((1,), (1,)), ((), ())), preferred_element_type=F32
        )

    for s in range(LIVE_MAX):
        product(s)

    for side, offset in ((0, -1), (1, 1)):
        source = me - offset

        @pl.when((source >= 0) & (source < devices))
        def _(copy=mig_copies[side]):
            copy.wait_recv()

    for s in [*range(early.stop, LIVE_MAX), *range(early.start)]:
        position = new_start + s
        left = mig_in[0, jnp.clip(position - old_start + MOVE, 0, MOVE - 1)]
        own = back_t[jnp.clip(position - old_start, 0, capacity - 1)]
        right = mig_in[1, jnp.clip(position - old_end, 0, MOVE - 1)]
        row = jnp.where(position < old_start, left, jnp.where(position < old_end, own, right))
        states[s, rank, :members] = row
    for piece in (last_piece, first_piece):
        send_own(piece, state_send, state_recv.at[0], state_recv.at[1])

    def pass_far(g):
        arrive_ahead(far[g], far_recv.at[0, g])
        send_passed(far[g], far_send.at[g], far_recv.at[1, g])

    def far_products(g):
        arrive_pair(far[g], far_recv.at[1, g])
        for c in range(HCAP):
            product(LIVE_MAX + g * HCAP + c)

    @pl.when(core == 0)
    def _():
        for g in range(HPEER):
            pass_far(g)
            far_products(g)

    @pl.when(core != 0)
    def _():
        for g in range(HPEER):
            pass_far(g)
        for g in range(HPEER):
            far_products(g)

    shape = (full, LANES)
    grid_row = lax.broadcasted_iota(jnp.int32, shape, 0)
    grid_col = lax.broadcasted_iota(jnp.int32, shape, 1)
    live_row = lax.rem(grid_row, PAD) < members
    live_col = (lax.rem(grid_col, PAD) < members) & (grid_col < full)
    rider = grid_row == members
    live = live_row & live_col
    kept = (live_row | rider) & live_col
    unit = jnp.where(live & (grid_row == grid_col), 1.0, 0.0)
    half_unit = 1.5 * unit
    shift = (ensemble - 1) / INFLATION
    entries = region_ref.shape[0]
    fill = jnp.zeros((LANES - full, LANES), BF16)

    def tall(a):
        return jnp.concatenate([a, fill], axis=0)

    def times(left, high, low):
        both = jnp.concatenate([high, high], axis=0)
        return dot(left, both) + dot(left[:, :LANES], low)

    def wide(a):
        high, low = cut(a)
        return jnp.concatenate([high, low], axis=1)

    norms = []
    for b in range(per_core):
        slot = jnp.minimum(CORES * b + core, LIVE_MAX - 1)
        gram = gram_s[slot]
        for e in range(entries):
            named = region_ref[e, slot]
            index = jnp.where(named < capacity, named, named - capacity + LIVE_MAX)
            index = jnp.clip(index, 0, LIVE_MAX + halo_count - 1)
            gram += weight_ref[e, slot] * gram_s[index]
        system = jnp.where(kept, gram, 0.0) + shift * unit
        square = jnp.where(live, system * system, 0.0)
        total = jnp.sum(jnp.sum(square, axis=1, keepdims=True), axis=0, keepdims=True)
        norm = jnp.sqrt(total)
        norms.append(norm)
        y = system / norm
        middle = half_unit - 0.5 * jnp.where(live, y, 0.0)
        high, low = cut(middle)
        first = times(wide(y), tall(high), tall(low))
        yz_s[b, :full] = wide(jnp.where(rider, 0.0, first))
        yz_s[b, full : 2 * full] = wide(jnp.where(rider, first, middle))

    def cross(b):
        z = yz_s[b, full : 2 * full]
        return times(z, yz_s[b, :LANES, :LANES], yz_s[b, :LANES, LANES:])

    def step(_, carry):
        middles = []
        for b in range(per_core):
            high, low = cut(half_unit - 0.5 * cross(b))
            middles.append((tall(high), tall(low)))
        for b in range(per_core):
            yz_s[b, : 2 * full] = wide(times(yz_s[b, : 2 * full], *middles[b]))
        return carry

    for k in range(NS_ITERS - 2):
        step(k, 0)

    piece = CORES * PAD
    block = 16
    start_row = members // block * block
    middles, riders = [], []
    for b in range(per_core):
        high, low = cut(half_unit - 0.5 * cross(b))
        middles.append((tall(high), tall(low)))
        q = yz_s[b, full + start_row : full + start_row + block]
        z_rows = slice(full, full + LANES)
        riders.append(times(q, yz_s[b, z_rows, :LANES], yz_s[b, z_rows, LANES:]))
    for b in range(per_core):
        chosen = yz_s[b, pl.ds(pl.multiple_of(full + chip * piece, block), piece)]
        stack = jnp.concatenate([chosen, wide(riders[b])], axis=0)
        both = times(stack, *middles[b])
        lead = times(wide(both[piece:]), *middles[b])[members - start_row : members - start_row + 1]
        spread = math.sqrt(ensemble - 1) * lax.rsqrt(norms[b])
        t_full[:, b] = (spread * both[:piece] + lead).astype(BF16).reshape(CORES, PAD, LANES)

    other = 1 - core
    t_copy = remote(t_full.at[other], t_all.at[core], t_send, t_recv, (me, pair))
    t_copy.start()
    t_all[core] = t_full[core]

    arrive_ahead(every_piece, state_recv.at[0])
    send_passed(every_piece, state_send, state_recv.at[1])
    arrive_pair(every_piece, state_recv.at[1])

    piece_row = lax.broadcasted_iota(jnp.int32, (PAD, full), 0)
    t_copy.wait_recv()
    for s in range(LIVE_MAX):
        weights = t_all[s % CORES, s // CORES][:, :full]
        weights = jnp.where(piece_row == members, jnp.ones_like(weights), weights)
        keep = 1.0 - jnp.sum(weights.astype(F32), axis=1, keepdims=True)
        blended = dot(weights, states[s].reshape(full, width))
        mean = blended[members : members + 1, :] / ensemble
        value = (blended + keep * mean)[:members]
        is_live = new_start + s < new_end
        out_ref[s] = jnp.where(is_live, value, 0.0).astype(BF16)
    for s in range(LIVE_MAX, capacity):
        out_ref[s] = jnp.zeros((members, width), BF16)

    for k, offset in enumerate(OFFSETS):
        target = me + offset

        @pl.when((target >= 0) & (target < devices))
        def _(copy=halo_copies[k]):
            copy.wait_send()

    for side, offset in ((0, -1), (1, 1)):
        target = me + offset

        @pl.when((target >= 0) & (target < devices))
        def _(copy=mig_copies[side]):
            copy.wait_send()

    t_copy.wait_send()
    whole_of(own_piece, load_sem.at[8], ranks - 1).wait()
    whole_of(every_piece, state_send, ranks - 1).wait()
    for g in range(HPEER):
        whole_of(far[g], far_send.at[g], ranks - 1).wait()


def shards(devices, ranks, background, obs_ens, innovation, precision, loc_weight, old_split,
           new_split, obs_count, halo_tiles, region_list):
    capacity, members, width = background.shape
    obs_slots = obs_ens.shape[2]
    full = PAD * ranks
    halo_count = HPEER * HCAP
    per_core = -(-LIVE_MAX // CORES)
    hbm = pl.BlockSpec(memory_space=pltpu.MemorySpace.HBM)
    vmem = pl.BlockSpec(memory_space=pltpu.VMEM)
    count = len(OFFSETS)
    dma = pltpu.SemaphoreType.DMA
    operands = (old_split, new_split, obs_count, halo_tiles, region_list.T, loc_weight.T,
                jnp.swapaxes(background, 0, 1), jnp.swapaxes(obs_ens, 0, 1), innovation, precision)
    spaces = [pltpu.SMEM] * 6 + [pltpu.VMEM] * 4
    return pl.pallas_call(
        functools.partial(kernel, devices, ranks),
        out_shape=pltpu.VMEM((capacity, members, width), BF16),
        in_specs=[hbm] * len(operands),
        out_specs=vmem,
        scratch_shapes=[space(x.shape, x.dtype) for space, x in zip(spaces, operands)] + [
            pltpu.VMEM((LIVE_MAX, PAD, obs_slots), BF16),
            pltpu.VMEM((capacity, members, width), BF16),
            pltpu.VMEM((LIVE_MAX + halo_count, ranks, PAD, obs_slots), BF16),
            pltpu.VMEM((count, HCAP, PAD, obs_slots), BF16),
            pltpu.VMEM((count, HCAP, PAD, obs_slots), BF16),
            pltpu.VMEM((2, MOVE, members, width), BF16),
            pltpu.VMEM((2, MOVE, members, width), BF16),
            pltpu.VMEM((LIVE_MAX, ranks, PAD, width), BF16),
            pltpu.VMEM((LIVE_MAX + halo_count, full, LANES), F32),
            pltpu.VMEM((per_core, full + LANES, 2 * LANES), BF16),
            pltpu.VMEM((CORES, per_core, PAD, LANES), BF16),
            pltpu.VMEM((CORES, per_core, PAD, LANES), BF16),
            dma((len(operands),)),
            dma((count,)),
            dma((2,)),
            dma((2,)),
            dma((HPEER,)),
            dma((2, HPEER)),
            dma,
            dma((2,)),
            dma,
            dma,
        ],
        compiler_params=pltpu.CompilerParams(
            collective_id=0, has_side_effects=True
        ),
        cost_estimate=pl.CostEstimate(flops=10**8, bytes_accessed=10**7, transcendentals=0),
    )(*operands)


def solution(mesh):
    in_specs = (
        P("tile", "mem", None),
        P("tile", "mem", None),
        P("tile", None),
        P("tile", None),
        P("tile", None),
        P(),
        P(),
        P("tile"),
        P(),
        P("tile", None),
    )
    out_specs = P("tile", "mem", None)
    body = functools.partial(shards, mesh.shape["tile"], mesh.shape["mem"])
    return jax.shard_map(body, mesh=mesh, in_specs=in_specs, out_specs=out_specs, check_vma=False)
```

```python
import functools
import math

import jax
import jax.numpy as jnp
from jax import lax
from jax.experimental import pallas as pl
from jax.experimental.pallas import tpu as pltpu
from jax.sharding import PartitionSpec as P

TILE_MEAN = 8
CORES = 2
MOVE = 2
REACH = 3
HPEER = 3
HCAP = 4
NS_ITERS = 6
LIVE_MAX = TILE_MEAN + MOVE
INFLATION = 1.1
PAD = 24
MESH = pl.DeviceIdType.MESH
F32 = jnp.float32
BF16 = jnp.bfloat16
LANES = 128
OFFSETS = tuple(range(-REACH, 0)) + tuple(range(1, REACH + 1))


def dot(a, b):
    return jnp.dot(a, b, preferred_element_type=F32)


def cut(a):
    high = a.astype(BF16)
    return high, (a - high.astype(F32)).astype(BF16)


def kernel(
    devices,
    ranks,
    old_hbm,
    new_hbm,
    count_hbm,
    halo_hbm,
    region_hbm,
    weight_hbm,
    back_hbm,
    obs_hbm,
    innov_hbm,
    prec_hbm,
    out_ref,
    old_ref,
    new_ref,
    count_ref,
    halo_ref,
    region_ref,
    weight_ref,
    back_ref,
    obs_ref,
    innov_ref,
    prec_ref,
    mine,
    back_t,
    table,
    stage,
    arrived,
    mig_out,
    mig_in,
    states,
    gram_s,
    yz_s,
    t_full,
    t_all,
    right_sem,
    load_sem,
    halo_recv,
    mig_recv,
    own_recv,
    far_send,
    far_recv,
    state_send,
    state_recv,
    t_send,
    t_recv,
):
    members, capacity, width = back_ref.shape
    obs_slots = obs_ref.shape[2]
    ensemble = members * ranks
    full = PAD * ranks
    halo_count = HPEER * HCAP
    per_core = -(-LIVE_MAX // CORES)
    me = lax.axis_index("tile")
    rank = lax.axis_index("mem")
    core = lax.rem(rank, CORES)
    chip = rank // CORES
    pair = rank + 1 - 2 * core
    half_ranks = ranks // CORES

    def signal(sem, tile, to):
        pl.semaphore_signal(sem, inc=1, device_id=(tile, to), device_id_type=MESH)

    barrier = pltpu.get_barrier_semaphore()
    for offset in range(1, REACH + 1):

        @pl.when(me + offset < devices)
        def _(offset=offset):
            signal(barrier, me + offset, rank)

    for j in range(1, ranks):
        signal(barrier, me, lax.rem(rank + j, ranks))

    loads = {}
    for k, (name, src, dst) in enumerate((
        ("count", count_hbm, count_ref),
        ("obs", obs_hbm, obs_ref),
        ("prec", prec_hbm, prec_ref),
        ("innov", innov_hbm, innov_ref),
        ("new", new_hbm, new_ref),
        ("halo", halo_hbm, halo_ref),
        ("back", back_hbm, back_ref),
        ("old", old_hbm, old_ref),
        ("region", region_hbm, region_ref),
        ("weight", weight_hbm, weight_ref),
    )):
        loads[name] = pltpu.make_async_copy(src, dst, load_sem.at[k])
        loads[name].start()

    pl.semaphore_wait(barrier, jnp.minimum(me, REACH) + ranks - 1)
    for offset in range(1, REACH + 1):

        @pl.when(me - offset >= 0)
        def _(offset=offset):
            signal(right_sem.at[offset - 1], me - offset, rank)

    row_id = lax.broadcasted_iota(jnp.int32, (PAD, obs_slots), 0)
    lane_id = lax.broadcasted_iota(jnp.int32, (1, obs_slots), 1)

    for s in range(LIVE_MAX):
        states[s, rank] = jnp.zeros((PAD, width), BF16)
    for b in range(per_core):
        yz_s[b, 2 * full :] = jnp.zeros((LANES - full, 2 * LANES), BF16)

    for name in ("count", "obs", "prec", "innov"):
        loads[name].wait()
    obs_all = obs_ref[...].astype(F32)
    for s in range(LIVE_MAX):
        live = (lane_id < count_ref[s]).astype(F32)
        root = jnp.sqrt(prec_ref[s : s + 1, :] * live)
        pulled = root * innov_ref[s : s + 1, :]
        rows = obs_all[:, s, :] * root
        fill = jnp.zeros((PAD - members, obs_slots), F32)
        block = jnp.concatenate([rows, fill], axis=0)
        block = jnp.where(row_id == members, pulled, block).astype(BF16)
        mine[s] = block
        table[s, rank] = block

    loads["new"].wait()
    loads["halo"].wait()
    loads["region"].wait()
    new_start, new_end = new_ref[me], new_ref[me + 1]
    def remote(src, dst, send, recv, target):
        return pltpu.make_async_remote_copy(
            src_ref=src,
            dst_ref=dst,
            send_sem=send,
            recv_sem=recv,
            device_id=target,
            device_id_type=MESH,
        )

    def fill_stage(k):
        reader = jnp.clip(me + OFFSETS[k], 0, devices - 1)
        for c in range(HCAP):
            index = jnp.int32(0)
            for g in range(HPEER):
                first = halo_ref[reader, g * HCAP]
                here = (first >= new_start) & (first < new_end)
                index += jnp.where(here, halo_ref[reader, g * HCAP + c] - new_start, 0)
            index = jnp.clip(index, 0, LIVE_MAX - 1)
            stage[k, c] = mine[index]

    halo_copies = []
    for k, offset in enumerate(OFFSETS):
        back_slot = len(OFFSETS) - 1 - k
        halo_copies.append(remote(
            stage.at[k], arrived.at[back_slot], load_sem.at[k], halo_recv.at[back_slot],
            (me + offset, rank),
        ))
    for k in range(REACH):
        fill_stage(k)

        @pl.when(me + OFFSETS[k] >= 0)
        def _(copy=halo_copies[k]):
            copy.start()

    for k in range(REACH, len(OFFSETS)):
        fill_stage(k)

    def send_own(piece, send, ahead_recv, pair_recv):
        here = piece(rank)
        for j in range(1, half_ranks):
            ahead = lax.rem(rank + CORES * j, ranks)
            remote(here, here, send, ahead_recv, (me, ahead)).start()
        remote(here, here, send, pair_recv, (me, pair)).start()

    def send_passed(piece, send, pair_recv):
        for j in range(1, half_ranks):
            behind = piece(lax.rem(rank + ranks - CORES * j, ranks))
            remote(behind, behind, send, pair_recv, (me, pair)).start()

    def whole_of(piece, sem, count):
        block = piece(pl.ds(0, count))
        return pltpu.make_async_copy(block, block, sem)

    def arrive_ahead(piece, sem):
        whole_of(piece, sem, half_ranks - 1).wait()

    def arrive_pair(piece, sem):
        whole_of(piece, sem, half_ranks).wait()

    def own_piece(r):
        return table.at[0:LIVE_MAX, r]

    send_own(own_piece, load_sem.at[8], own_recv.at[0], own_recv.at[1])

    loads["back"].wait()
    loads["old"].wait()
    loads["weight"].wait()
    old_start, old_end = old_ref[me], old_ref[me + 1]
    back_all = back_ref[...].astype(F32)
    for s in range(capacity):
        back_t[s] = back_all[:, s, :].astype(BF16)
    old_count = old_end - old_start
    for c in range(MOVE):
        mig_out[0, c] = back_t[jnp.clip(c, 0, capacity - 1)]
        mig_out[1, c] = back_t[jnp.clip(old_count - MOVE + c, 0, capacity - 1)]
    mig_copies = []
    for side, offset in ((0, -1), (1, 1)):
        target = me + offset
        copy = remote(
            mig_out.at[side], mig_in.at[1 - side], load_sem.at[len(OFFSETS) + side], mig_recv.at[1 - side],
            (target, rank),
        )
        mig_copies.append(copy)

    @pl.when(me > 0)
    def _():
        mig_copies[0].start()

    early = range(MOVE, TILE_MEAN - 2 * MOVE)
    for s in early:
        states[s, rank, :members] = back_t[jnp.clip(new_start + s - old_start, 0, capacity - 1)]

    def early_piece(r):
        return states.at[early.start : early.stop, r]

    def first_piece(r):
        return states.at[0 : early.start, r]

    def last_piece(r):
        return states.at[early.stop : LIVE_MAX, r]

    def every_piece(r):
        return states.at[0:LIVE_MAX, r]

    send_own(early_piece, state_send, state_recv.at[0], state_recv.at[1])

    for offset in range(1, REACH + 1):

        @pl.when(me + offset < devices)
        def _(offset=offset):
            pl.semaphore_wait(right_sem.at[offset - 1], 1)
            halo_copies[OFFSETS.index(offset)].start()
            if offset == 1:
                mig_copies[1].start()


    for k, offset in enumerate(OFFSETS):
        back_slot = len(OFFSETS) - 1 - k
        source = me + OFFSETS[back_slot]

        @pl.when((source >= 0) & (source < devices))
        def _(copy=halo_copies[k]):
            copy.wait_recv()

    far = []
    for g in range(HPEER):
        first = halo_ref[me, g * HCAP]
        owner = jnp.int32(0)
        for k, offset in enumerate(OFFSETS):
            source = jnp.clip(me + offset, 0, devices - 1)
            held = (first >= new_ref[source]) & (first < new_ref[source + 1])
            inside = (me + offset >= 0) & (me + offset < devices)
            owner = jnp.where(held & inside, k, owner)
        for c in range(HCAP):
            table[LIVE_MAX + g * HCAP + c, rank] = arrived[owner, c]
        first_row = LIVE_MAX + g * HCAP

        def far_piece(r, first_row=first_row):
            return table.at[first_row : first_row + HCAP, r]

        far.append(far_piece)
        send_own(far_piece, far_send.at[g], far_recv.at[0, g], far_recv.at[1, g])

    arrive_ahead(own_piece, own_recv.at[0])
    send_passed(own_piece, load_sem.at[8], own_recv.at[1])
    arrive_pair(own_piece, own_recv.at[1])

    blank = jnp.zeros((LANES - full, obs_slots), BF16)

    def product(index):
        block = table[index].reshape(full, obs_slots)
        wide = jnp.concatenate([block, blank], axis=0)
        gram_s[index] = lax.dot_general(
            block, wide, (((1,), (1,)), ((), ())), preferred_element_type=F32
        )

    for s in range(LIVE_MAX):
        product(s)

    for side, offset in ((0, -1), (1, 1)):
        source = me - offset

        @pl.when((source >= 0) & (source < devices))
        def _(copy=mig_copies[side]):
            copy.wait_recv()

    for s in [*range(early.stop, LIVE_MAX), *range(early.start)]:
        position = new_start + s
        left = mig_in[0, jnp.clip(position - old_start + MOVE, 0, MOVE - 1)]
        own = back_t[jnp.clip(position - old_start, 0, capacity - 1)]
        right = mig_in[1, jnp.clip(position - old_end, 0, MOVE - 1)]
        row = jnp.where(position < old_start, left, jnp.where(position < old_end, own, right))
        states[s, rank, :members] = row
    for piece in (last_piece, first_piece):
        send_own(piece, state_send, state_recv.at[0], state_recv.at[1])

    def pass_far(g):
        arrive_ahead(far[g], far_recv.at[0, g])
        send_passed(far[g], far_send.at[g], far_recv.at[1, g])

    def far_products(g):
        arrive_pair(far[g], far_recv.at[1, g])
        for c in range(HCAP):
            product(LIVE_MAX + g * HCAP + c)

    @pl.when(core == 0)
    def _():
        for g in range(HPEER):
            pass_far(g)
            far_products(g)

    @pl.when(core != 0)
    def _():
        for g in range(HPEER):
            pass_far(g)
        for g in range(HPEER):
            far_products(g)

    shape = (full, LANES)
    grid_row = lax.broadcasted_iota(jnp.int32, shape, 0)
    grid_col = lax.broadcasted_iota(jnp.int32, shape, 1)
    live_row = lax.rem(grid_row, PAD) < members
    live_col = (lax.rem(grid_col, PAD) < members) & (grid_col < full)
    rider = grid_row == members
    live = live_row & live_col
    kept = (live_row | rider) & live_col
    unit = jnp.where(live & (grid_row == grid_col), 1.0, 0.0)
    half_unit = 1.5 * unit
    shift = (ensemble - 1) / INFLATION
    entries = region_ref.shape[0]
    fill = jnp.zeros((LANES - full, LANES), BF16)

    def tall(a):
        return jnp.concatenate([a, fill], axis=0)

    def times(left, high, low):
        both = jnp.concatenate([high, high], axis=0)
        return dot(left, both) + dot(left[:, :LANES], low)

    def wide(a):
        high, low = cut(a)
        return jnp.concatenate([high, low], axis=1)

    norms = []
    for b in range(per_core):
        slot = jnp.minimum(CORES * b + core, LIVE_MAX - 1)
        gram = gram_s[slot]
        for e in range(entries):
            named = region_ref[e, slot]
            index = jnp.where(named < capacity, named, named - capacity + LIVE_MAX)
            index = jnp.clip(index, 0, LIVE_MAX + halo_count - 1)
            gram += weight_ref[e, slot] * gram_s[index]
        system = jnp.where(kept, gram, 0.0) + shift * unit
        square = jnp.where(live, system * system, 0.0)
        total = jnp.sum(jnp.sum(square, axis=1, keepdims=True), axis=0, keepdims=True)
        norm = jnp.sqrt(total)
        norms.append(norm)
        y = system / norm
        middle = half_unit - 0.5 * jnp.where(live, y, 0.0)
        high, low = cut(middle)
        first = times(wide(y), tall(high), tall(low))
        yz_s[b, :full] = wide(jnp.where(rider, 0.0, first))
        yz_s[b, full : 2 * full] = wide(jnp.where(rider, first, middle))

    def cross(b):
        z = yz_s[b, full : 2 * full]
        return times(z, yz_s[b, :LANES, :LANES], yz_s[b, :LANES, LANES:])

    def step(_, carry):
        middles = []
        for b in range(per_core):
            high, low = cut(half_unit - 0.5 * cross(b))
            middles.append((tall(high), tall(low)))
        for b in range(per_core):
            yz_s[b, : 2 * full] = wide(times(yz_s[b, : 2 * full], *middles[b]))
        return carry

    for k in range(NS_ITERS - 2):
        step(k, 0)

    piece = CORES * PAD
    block = 16
    start_row = members // block * block
    middles, riders = [], []
    for b in range(per_core):
        high, low = cut(half_unit - 0.5 * cross(b))
        middles.append((tall(high), tall(low)))
        q = yz_s[b, full + start_row : full + start_row + block]
        z_rows = slice(full, full + LANES)
        riders.append(times(q, yz_s[b, z_rows, :LANES], yz_s[b, z_rows, LANES:]))
    for b in range(per_core):
        chosen = yz_s[b, pl.ds(pl.multiple_of(full + chip * piece, block), piece)]
        stack = jnp.concatenate([chosen, wide(riders[b])], axis=0)
        both = times(stack, *middles[b])
        lead = times(wide(both[piece:]), *middles[b])[members - start_row : members - start_row + 1]
        spread = math.sqrt(ensemble - 1) * lax.rsqrt(norms[b])
        t_full[:, b] = (spread * both[:piece] + lead).astype(BF16).reshape(CORES, PAD, LANES)

    other = 1 - core
    t_copy = remote(t_full.at[other], t_all.at[core], t_send, t_recv, (me, pair))
    t_copy.start()
    t_all[core] = t_full[core]

    arrive_ahead(every_piece, state_recv.at[0])
    send_passed(every_piece, state_send, state_recv.at[1])
    arrive_pair(every_piece, state_recv.at[1])

    piece_row = lax.broadcasted_iota(jnp.int32, (PAD, full), 0)
    t_copy.wait_recv()
    for s in range(LIVE_MAX):
        weights = t_all[s % CORES, s // CORES][:, :full]
        weights = jnp.where(piece_row == members, jnp.ones_like(weights), weights)
        keep = 1.0 - jnp.sum(weights.astype(F32), axis=1, keepdims=True)
        blended = dot(weights, states[s].reshape(full, width))
        mean = blended[members : members + 1, :] / ensemble
        value = (blended + keep * mean)[:members]
        is_live = new_start + s < new_end
        out_ref[s] = jnp.where(is_live, value, 0.0).astype(BF16)
    for s in range(LIVE_MAX, capacity):
        out_ref[s] = jnp.zeros((members, width), BF16)

    for k, offset in enumerate(OFFSETS):
        target = me + offset

        @pl.when((target >= 0) & (target < devices))
        def _(copy=halo_copies[k]):
            copy.wait_send()

    for side, offset in ((0, -1), (1, 1)):
        target = me + offset

        @pl.when((target >= 0) & (target < devices))
        def _(copy=mig_copies[side]):
            copy.wait_send()

    t_copy.wait_send()
    whole_of(own_piece, load_sem.at[8], ranks - 1).wait()
    whole_of(every_piece, state_send, ranks - 1).wait()
    for g in range(HPEER):
        whole_of(far[g], far_send.at[g], ranks - 1).wait()


def shards(devices, ranks, background, obs_ens, innovation, precision, loc_weight, old_split,
           new_split, obs_count, halo_tiles, region_list):
    capacity, members, width = background.shape
    obs_slots = obs_ens.shape[2]
    full = PAD * ranks
    halo_count = HPEER * HCAP
    per_core = -(-LIVE_MAX // CORES)
    hbm = pl.BlockSpec(memory_space=pltpu.MemorySpace.HBM)
    vmem = pl.BlockSpec(memory_space=pltpu.VMEM)
    count = len(OFFSETS)
    dma = pltpu.SemaphoreType.DMA
    operands = (old_split, new_split, obs_count, halo_tiles, region_list.T, loc_weight.T,
                jnp.swapaxes(background, 0, 1), jnp.swapaxes(obs_ens, 0, 1), innovation, precision)
    spaces = [pltpu.SMEM] * 6 + [pltpu.VMEM] * 4
    return pl.pallas_call(
        functools.partial(kernel, devices, ranks),
        out_shape=pltpu.VMEM((capacity, members, width), BF16),
        in_specs=[hbm] * len(operands),
        out_specs=vmem,
        scratch_shapes=[space(x.shape, x.dtype) for space, x in zip(spaces, operands)] + [
            pltpu.VMEM((LIVE_MAX, PAD, obs_slots), BF16),
            pltpu.VMEM((capacity, members, width), BF16),
            pltpu.VMEM((LIVE_MAX + halo_count, ranks, PAD, obs_slots), BF16),
            pltpu.VMEM((count, HCAP, PAD, obs_slots), BF16),
            pltpu.VMEM((count, HCAP, PAD, obs_slots), BF16),
            pltpu.VMEM((2, MOVE, members, width), BF16),
            pltpu.VMEM((2, MOVE, members, width), BF16),
            pltpu.VMEM((LIVE_MAX, ranks, PAD, width), BF16),
            pltpu.VMEM((LIVE_MAX + halo_count, full, LANES), F32),
            pltpu.VMEM((per_core, full + LANES, 2 * LANES), BF16),
            pltpu.VMEM((CORES, per_core, PAD, LANES), BF16),
            pltpu.VMEM((CORES, per_core, PAD, LANES), BF16),
            pltpu.SemaphoreType.REGULAR((REACH,)),
            dma((len(operands),)),
            dma((count,)),
            dma((2,)),
            dma((2,)),
            dma((HPEER,)),
            dma((2, HPEER)),
            dma,
            dma((2,)),
            dma,
            dma,
        ],
        compiler_params=pltpu.CompilerParams(
            collective_id=0, has_side_effects=True
        ),
        cost_estimate=pl.CostEstimate(flops=10**8, bytes_accessed=10**7, transcendentals=0),
    )(*operands)


def solution(mesh):
    in_specs = (
        P("tile", "mem", None),
        P("tile", "mem", None),
        P("tile", None),
        P("tile", None),
        P("tile", None),
        P(),
        P(),
        P("tile"),
        P(),
        P("tile", None),
    )
    out_specs = P("tile", "mem", None)
    body = functools.partial(shards, mesh.shape["tile"], mesh.shape["mem"])
    return jax.shard_map(body, mesh=mesh, in_specs=in_specs, out_specs=out_specs, check_vma=False)
```

```python
import functools
import math

import jax
import jax.numpy as jnp
from jax import lax
from jax.experimental import pallas as pl
from jax.experimental.pallas import tpu as pltpu
from jax.sharding import PartitionSpec as P

TILE_MEAN = 8
CORES = 2
MOVE = 2
REACH = 3
HPEER = 3
HCAP = 4
NS_ITERS = 6
LIVE_MAX = TILE_MEAN + MOVE
INFLATION = 1.1
PAD = 24
MESH = pl.DeviceIdType.MESH
F32 = jnp.float32
BF16 = jnp.bfloat16
LANES = 128
SPLIT = 6
OFFSETS = tuple(range(-REACH, 0)) + tuple(range(1, REACH + 1))


def dot(a, b):
    return jnp.dot(a, b, preferred_element_type=F32)


def cut(a):
    high = a.astype(BF16)
    return high, (a - high.astype(F32)).astype(BF16)


def kernel(
    devices,
    ranks,
    old_hbm,
    new_hbm,
    count_hbm,
    halo_hbm,
    region_hbm,
    weight_hbm,
    back_hbm,
    obs_hbm,
    innov_hbm,
    prec_hbm,
    out_ref,
    old_ref,
    new_ref,
    count_ref,
    halo_ref,
    region_ref,
    weight_ref,
    back_ref,
    obs_ref,
    innov_ref,
    prec_ref,
    mine,
    back_t,
    table,
    stage,
    arrived,
    mig_out,
    mig_in,
    states,
    gram_s,
    yz_s,
    t_full,
    t_all,
    right_sem,
    load_sem,
    halo_recv,
    mig_recv,
    own_recv,
    far_send,
    far_recv,
    state_send,
    state_recv,
    t_send,
    t_recv,
):
    members, capacity, width = back_ref.shape
    obs_slots = obs_ref.shape[2]
    ensemble = members * ranks
    full = PAD * ranks
    halo_count = HPEER * HCAP
    per_core = max(SPLIT, LIVE_MAX - SPLIT)
    me = lax.axis_index("tile")
    rank = lax.axis_index("mem")
    core = lax.rem(rank, CORES)
    chip = rank // CORES
    pair = rank + 1 - 2 * core
    half_ranks = ranks // CORES

    def signal(sem, tile, to):
        pl.semaphore_signal(sem, inc=1, device_id=(tile, to), device_id_type=MESH)

    barrier = pltpu.get_barrier_semaphore()
    for offset in range(1, REACH + 1):

        @pl.when(me + offset < devices)
        def _(offset=offset):
            signal(barrier, me + offset, rank)

    for j in range(1, ranks):
        signal(barrier, me, lax.rem(rank + j, ranks))

    loads = {}
    for k, (name, src, dst) in enumerate((
        ("count", count_hbm, count_ref),
        ("obs", obs_hbm, obs_ref),
        ("prec", prec_hbm, prec_ref),
        ("innov", innov_hbm, innov_ref),
        ("new", new_hbm, new_ref),
        ("halo", halo_hbm, halo_ref),
        ("back", back_hbm, back_ref),
        ("old", old_hbm, old_ref),
        ("region", region_hbm, region_ref),
        ("weight", weight_hbm, weight_ref),
    )):
        loads[name] = pltpu.make_async_copy(src, dst, load_sem.at[k])
        loads[name].start()

    pl.semaphore_wait(barrier, jnp.minimum(me, REACH) + ranks - 1)
    for offset in range(1, REACH + 1):

        @pl.when(me - offset >= 0)
        def _(offset=offset):
            signal(right_sem.at[offset - 1], me - offset, rank)

    row_id = lax.broadcasted_iota(jnp.int32, (PAD, obs_slots), 0)
    lane_id = lax.broadcasted_iota(jnp.int32, (1, obs_slots), 1)

    for s in range(LIVE_MAX):
        states[s, rank] = jnp.zeros((PAD, width), BF16)
    for b in range(per_core):
        yz_s[b, 2 * full :] = jnp.zeros((LANES - full, 2 * LANES), BF16)

    for name in ("count", "obs", "prec", "innov"):
        loads[name].wait()
    obs_all = obs_ref[...].astype(F32)
    for s in range(LIVE_MAX):
        live = (lane_id < count_ref[s]).astype(F32)
        root = jnp.sqrt(prec_ref[s : s + 1, :] * live)
        pulled = root * innov_ref[s : s + 1, :]
        rows = obs_all[:, s, :] * root
        fill = jnp.zeros((PAD - members, obs_slots), F32)
        block = jnp.concatenate([rows, fill], axis=0)
        block = jnp.where(row_id == members, pulled, block).astype(BF16)
        mine[s] = block
        table[s, rank] = block

    loads["new"].wait()
    loads["halo"].wait()
    loads["region"].wait()
    new_start, new_end = new_ref[me], new_ref[me + 1]
    def remote(src, dst, send, recv, target):
        return pltpu.make_async_remote_copy(
            src_ref=src,
            dst_ref=dst,
            send_sem=send,
            recv_sem=recv,
            device_id=target,
            device_id_type=MESH,
        )

    def fill_stage(k):
        reader = jnp.clip(me + OFFSETS[k], 0, devices - 1)
        for c in range(HCAP):
            index = jnp.int32(0)
            for g in range(HPEER):
                first = halo_ref[reader, g * HCAP]
                here = (first >= new_start) & (first < new_end)
                index += jnp.where(here, halo_ref[reader, g * HCAP + c] - new_start, 0)
            index = jnp.clip(index, 0, LIVE_MAX - 1)
            stage[k, c] = mine[index]

    halo_copies = []
    for k, offset in enumerate(OFFSETS):
        back_slot = len(OFFSETS) - 1 - k
        halo_copies.append(remote(
            stage.at[k], arrived.at[back_slot], load_sem.at[k], halo_recv.at[back_slot],
            (me + offset, rank),
        ))
    for k in range(REACH):
        fill_stage(k)

        @pl.when(me + OFFSETS[k] >= 0)
        def _(copy=halo_copies[k]):
            copy.start()

    for k in range(REACH, len(OFFSETS)):
        fill_stage(k)

    def send_own(piece, send, ahead_recv, pair_recv):
        here = piece(rank)
        for j in range(1, half_ranks):
            ahead = lax.rem(rank + CORES * j, ranks)
            remote(here, here, send, ahead_recv, (me, ahead)).start()
        remote(here, here, send, pair_recv, (me, pair)).start()

    def send_passed(piece, send, pair_recv):
        for j in range(1, half_ranks):
            behind = piece(lax.rem(rank + ranks - CORES * j, ranks))
            remote(behind, behind, send, pair_recv, (me, pair)).start()

    def whole_of(piece, sem, count):
        block = piece(pl.ds(0, count))
        return pltpu.make_async_copy(block, block, sem)

    def arrive_ahead(piece, sem):
        whole_of(piece, sem, half_ranks - 1).wait()

    def arrive_pair(piece, sem):
        whole_of(piece, sem, half_ranks).wait()

    def own_piece(r):
        return table.at[0:LIVE_MAX, r]

    send_own(own_piece, load_sem.at[8], own_recv.at[0], own_recv.at[1])

    loads["back"].wait()
    loads["old"].wait()
    loads["weight"].wait()
    old_start, old_end = old_ref[me], old_ref[me + 1]
    back_all = back_ref[...].astype(F32)
    for s in range(capacity):
        back_t[s] = back_all[:, s, :].astype(BF16)
    old_count = old_end - old_start
    for c in range(MOVE):
        mig_out[0, c] = back_t[jnp.clip(c, 0, capacity - 1)]
        mig_out[1, c] = back_t[jnp.clip(old_count - MOVE + c, 0, capacity - 1)]
    mig_copies = []
    for side, offset in ((0, -1), (1, 1)):
        target = me + offset
        copy = remote(
            mig_out.at[side], mig_in.at[1 - side], load_sem.at[len(OFFSETS) + side], mig_recv.at[1 - side],
            (target, rank),
        )
        mig_copies.append(copy)

    @pl.when(me > 0)
    def _():
        mig_copies[0].start()

    early = range(MOVE, TILE_MEAN - 2 * MOVE)
    for s in early:
        states[s, rank, :members] = back_t[jnp.clip(new_start + s - old_start, 0, capacity - 1)]

    def early_piece(r):
        return states.at[early.start : early.stop, r]

    def first_piece(r):
        return states.at[0 : early.start, r]

    def last_piece(r):
        return states.at[early.stop : LIVE_MAX, r]

    def every_piece(r):
        return states.at[0:LIVE_MAX, r]

    send_own(early_piece, state_send, state_recv.at[0], state_recv.at[1])

    for offset in range(1, REACH + 1):

        @pl.when(me + offset < devices)
        def _(offset=offset):
            pl.semaphore_wait(right_sem.at[offset - 1], 1)
            halo_copies[OFFSETS.index(offset)].start()
            if offset == 1:
                mig_copies[1].start()


    for k, offset in enumerate(OFFSETS):
        back_slot = len(OFFSETS) - 1 - k
        source = me + OFFSETS[back_slot]

        @pl.when((source >= 0) & (source < devices))
        def _(copy=halo_copies[k]):
            copy.wait_recv()

    far = []
    for g in range(HPEER):
        first = halo_ref[me, g * HCAP]
        owner = jnp.int32(0)
        for k, offset in enumerate(OFFSETS):
            source = jnp.clip(me + offset, 0, devices - 1)
            held = (first >= new_ref[source]) & (first < new_ref[source + 1])
            inside = (me + offset >= 0) & (me + offset < devices)
            owner = jnp.where(held & inside, k, owner)
        for c in range(HCAP):
            table[LIVE_MAX + g * HCAP + c, rank] = arrived[owner, c]
        first_row = LIVE_MAX + g * HCAP

        def far_piece(r, first_row=first_row):
            return table.at[first_row : first_row + HCAP, r]

        far.append(far_piece)
        send_own(far_piece, far_send.at[g], far_recv.at[0, g], far_recv.at[1, g])

    arrive_ahead(own_piece, own_recv.at[0])
    send_passed(own_piece, load_sem.at[8], own_recv.at[1])

    blank = jnp.zeros((LANES - full, obs_slots), BF16)

    def product(index):
        block = table[index].reshape(full, obs_slots)
        wide = jnp.concatenate([block, blank], axis=0)
        gram_s[index] = lax.dot_general(
            block, wide, (((1,), (1,)), ((), ())), preferred_element_type=F32
        )

    def own_products():
        arrive_pair(own_piece, own_recv.at[1])
        for s in range(LIVE_MAX):
            product(s)

    def send_states():
        for side, offset in ((0, -1), (1, 1)):
            source = me - offset

            @pl.when((source >= 0) & (source < devices))
            def _(copy=mig_copies[side]):
                copy.wait_recv()

        for s in [*range(early.stop, LIVE_MAX), *range(early.start)]:
            position = new_start + s
            left = mig_in[0, jnp.clip(position - old_start + MOVE, 0, MOVE - 1)]
            own = back_t[jnp.clip(position - old_start, 0, capacity - 1)]
            right = mig_in[1, jnp.clip(position - old_end, 0, MOVE - 1)]
            row = jnp.where(position < old_start, left, jnp.where(position < old_end, own, right))
            states[s, rank, :members] = row
        for piece in (last_piece, first_piece):
            send_own(piece, state_send, state_recv.at[0], state_recv.at[1])

    def pass_far(g):
        arrive_ahead(far[g], far_recv.at[0, g])
        send_passed(far[g], far_send.at[g], far_recv.at[1, g])

    def far_products(g):
        arrive_pair(far[g], far_recv.at[1, g])
        for c in range(HCAP):
            product(LIVE_MAX + g * HCAP + c)

    @pl.when(core == 0)
    def _():
        own_products()
        send_states()
        for g in range(HPEER):
            pass_far(g)
            far_products(g)

    @pl.when(core != 0)
    def _():
        for g in range(HPEER):
            pass_far(g)
        own_products()
        send_states()
        for g in range(HPEER):
            far_products(g)

    shape = (full, LANES)
    grid_row = lax.broadcasted_iota(jnp.int32, shape, 0)
    grid_col = lax.broadcasted_iota(jnp.int32, shape, 1)
    live_row = lax.rem(grid_row, PAD) < members
    live_col = (lax.rem(grid_col, PAD) < members) & (grid_col < full)
    rider = grid_row == members
    live = live_row & live_col
    kept = (live_row | rider) & live_col
    unit = jnp.where(live & (grid_row == grid_col), 1.0, 0.0)
    half_unit = 1.5 * unit
    shift = (ensemble - 1) / INFLATION
    entries = region_ref.shape[0]
    fill = jnp.zeros((LANES - full, LANES), BF16)

    def tall(a):
        return jnp.concatenate([a, fill], axis=0)

    def times(left, high, low):
        both = jnp.concatenate([high, high], axis=0)
        return dot(left, both) + dot(left[:, :LANES], low)

    def wide(a):
        high, low = cut(a)
        return jnp.concatenate([high, low], axis=1)

    def solve(first_slot, count):
        norms = []
        for b in range(count):
            slot = first_slot + b
            gram = gram_s[slot]
            for e in range(entries):
                named = region_ref[e, slot]
                index = jnp.where(named < capacity, named, named - capacity + LIVE_MAX)
                index = jnp.clip(index, 0, LIVE_MAX + halo_count - 1)
                gram += weight_ref[e, slot] * gram_s[index]
            system = jnp.where(kept, gram, 0.0) + shift * unit
            square = jnp.where(live, system * system, 0.0)
            total = jnp.sum(jnp.sum(square, axis=1, keepdims=True), axis=0, keepdims=True)
            norm = jnp.sqrt(total)
            norms.append(norm)
            high, low = cut(jnp.where(live, system, 0.0))
            squared = times(wide(system), tall(high), tall(low))
            scale = 1.0 / norm
            y = system * scale
            middle = half_unit - 0.5 * jnp.where(live, y, 0.0)
            first = 1.5 * y - (0.5 * scale * scale) * squared
            yz_s[b, :full] = wide(jnp.where(rider, 0.0, first))
            yz_s[b, full : 2 * full] = wide(jnp.where(rider, first, middle))

        def cross(b):
            z = yz_s[b, full : 2 * full]
            return times(z, yz_s[b, :LANES, :LANES], yz_s[b, :LANES, LANES:])

        def step(_, carry):
            middles = []
            for b in range(count):
                high, low = cut(half_unit - 0.5 * cross(b))
                middles.append((tall(high), tall(low)))
            for b in range(count):
                yz_s[b, : 2 * full] = wide(times(yz_s[b, : 2 * full], *middles[b]))
            return carry

        for k in range(NS_ITERS - 2):
            step(k, 0)

        piece = CORES * PAD
        block = 16
        start_row = members // block * block
        middles, riders = [], []
        for b in range(count):
            high, low = cut(half_unit - 0.5 * cross(b))
            middles.append((tall(high), tall(low)))
            q = yz_s[b, full + start_row : full + start_row + block]
            z_rows = slice(full, full + LANES)
            riders.append(times(q, yz_s[b, z_rows, :LANES], yz_s[b, z_rows, LANES:]))
        for b in range(count):
            chosen = yz_s[b, pl.ds(pl.multiple_of(full + chip * piece, block), piece)]
            stack = jnp.concatenate([chosen, wide(riders[b])], axis=0)
            both = times(stack, *middles[b])
            lead = times(wide(both[piece:]), *middles[b])[members - start_row : members - start_row + 1]
            spread = math.sqrt(ensemble - 1) * lax.rsqrt(norms[b])
            t_full[:, first_slot + b] = (spread * both[:piece] + lead).astype(BF16).reshape(CORES, PAD, LANES)

    def exchange(core_from):
        rows = (0, SPLIT) if core_from == 0 else (SPLIT, LIVE_MAX)
        target = t_full.at[1 - core_from, rows[0] : rows[1]]
        return remote(target, t_all.at[rows[0] : rows[1]], t_send, t_recv, (me, pair))

    @pl.when(core == 0)
    def _():
        solve(0, SPLIT)
        exchange(0).start()
        t_all[0:SPLIT] = t_full[0, 0:SPLIT]

    @pl.when(core != 0)
    def _():
        solve(SPLIT, LIVE_MAX - SPLIT)
        exchange(1).start()
        t_all[SPLIT:LIVE_MAX] = t_full[1, SPLIT:LIVE_MAX]

    arrive_ahead(every_piece, state_recv.at[0])
    send_passed(every_piece, state_send, state_recv.at[1])
    arrive_pair(every_piece, state_recv.at[1])

    piece_row = lax.broadcasted_iota(jnp.int32, (PAD, full), 0)

    @pl.when(core == 0)
    def _():
        exchange(1).wait_recv()

    @pl.when(core != 0)
    def _():
        exchange(0).wait_recv()

    for s in range(LIVE_MAX):
        weights = t_all[s][:, :full]
        weights = jnp.where(piece_row == members, jnp.ones_like(weights), weights)
        keep = 1.0 - jnp.sum(weights.astype(F32), axis=1, keepdims=True)
        blended = dot(weights, states[s].reshape(full, width))
        mean = blended[members : members + 1, :] / ensemble
        value = (blended + keep * mean)[:members]
        is_live = new_start + s < new_end
        out_ref[s] = jnp.where(is_live, value, 0.0).astype(BF16)
    for s in range(LIVE_MAX, capacity):
        out_ref[s] = jnp.zeros((members, width), BF16)

    for k, offset in enumerate(OFFSETS):
        target = me + offset

        @pl.when((target >= 0) & (target < devices))
        def _(copy=halo_copies[k]):
            copy.wait_send()

    for side, offset in ((0, -1), (1, 1)):
        target = me + offset

        @pl.when((target >= 0) & (target < devices))
        def _(copy=mig_copies[side]):
            copy.wait_send()


    @pl.when(core == 0)
    def _():
        exchange(0).wait_send()

    @pl.when(core != 0)
    def _():
        exchange(1).wait_send()

    whole_of(own_piece, load_sem.at[8], ranks - 1).wait()
    whole_of(every_piece, state_send, ranks - 1).wait()
    for g in range(HPEER):
        whole_of(far[g], far_send.at[g], ranks - 1).wait()


def shards(devices, ranks, background, obs_ens, innovation, precision, loc_weight, old_split,
           new_split, obs_count, halo_tiles, region_list):
    capacity, members, width = background.shape
    obs_slots = obs_ens.shape[2]
    full = PAD * ranks
    halo_count = HPEER * HCAP
    per_core = max(SPLIT, LIVE_MAX - SPLIT)
    hbm = pl.BlockSpec(memory_space=pltpu.MemorySpace.HBM)
    vmem = pl.BlockSpec(memory_space=pltpu.VMEM)
    count = len(OFFSETS)
    dma = pltpu.SemaphoreType.DMA
    operands = (old_split, new_split, obs_count, halo_tiles, region_list.T, loc_weight.T,
                jnp.swapaxes(background, 0, 1), jnp.swapaxes(obs_ens, 0, 1), innovation, precision)
    spaces = [pltpu.SMEM] * 6 + [pltpu.VMEM] * 4
    return pl.pallas_call(
        functools.partial(kernel, devices, ranks),
        out_shape=pltpu.VMEM((capacity, members, width), BF16),
        in_specs=[hbm] * len(operands),
        out_specs=vmem,
        scratch_shapes=[space(x.shape, x.dtype) for space, x in zip(spaces, operands)] + [
            pltpu.VMEM((LIVE_MAX, PAD, obs_slots), BF16),
            pltpu.VMEM((capacity, members, width), BF16),
            pltpu.VMEM((LIVE_MAX + halo_count, ranks, PAD, obs_slots), BF16),
            pltpu.VMEM((count, HCAP, PAD, obs_slots), BF16),
            pltpu.VMEM((count, HCAP, PAD, obs_slots), BF16),
            pltpu.VMEM((2, MOVE, members, width), BF16),
            pltpu.VMEM((2, MOVE, members, width), BF16),
            pltpu.VMEM((LIVE_MAX, ranks, PAD, width), BF16),
            pltpu.VMEM((LIVE_MAX + halo_count, full, LANES), F32),
            pltpu.VMEM((per_core, full + LANES, 2 * LANES), BF16),
            pltpu.VMEM((CORES, LIVE_MAX, PAD, LANES), BF16),
            pltpu.VMEM((LIVE_MAX, PAD, LANES), BF16),
            pltpu.SemaphoreType.REGULAR((REACH,)),
            dma((len(operands),)),
            dma((count,)),
            dma((2,)),
            dma((2,)),
            dma((HPEER,)),
            dma((2, HPEER)),
            dma,
            dma((2,)),
            dma,
            dma,
        ],
        compiler_params=pltpu.CompilerParams(
            collective_id=0, has_side_effects=True
        ),
        cost_estimate=pl.CostEstimate(flops=10**8, bytes_accessed=10**7, transcendentals=0),
    )(*operands)


def solution(mesh):
    in_specs = (
        P("tile", "mem", None),
        P("tile", "mem", None),
        P("tile", None),
        P("tile", None),
        P("tile", None),
        P(),
        P(),
        P("tile"),
        P(),
        P("tile", None),
    )
    out_specs = P("tile", "mem", None)
    body = functools.partial(shards, mesh.shape["tile"], mesh.shape["mem"])
    return jax.shard_map(body, mesh=mesh, in_specs=in_specs, out_specs=out_specs, check_vma=False)
```
